32 devices in a mesh: data: 32 (over z, y, x, core).
Axes of the slice: x: 2, y: 2, z: 4, core: 2. Of those that a mesh axis runs over, the one named last changes fastest.
Arguments:
- x_in: bfloat16 [1024, 16, 256], P('data')
- targets: int32 [1024, 16], P('data')
- w_lstm: bfloat16 [8, 512, 1024], replicated
- b_lstm: float32 [8, 1024], replicated
- w_vocab: bfloat16 [256, 32000], replicated
Outputs:
- output 1: float32 [8, 512, 1024], replicated
- output 2: float32 [8, 1024], replicated
- output 3: float32 [256, 32000], replicated
- output 4: float32 [1024, 16, 256], P('data')
All inputs are finite; a program needn't handle non-finite values.
Results may differ from the reference program's by a relative error of at most 0.00384.
Values are sent between devices in bfloat16 or wider.
A program may use at most 1 GiB of HBM per device.

```python
import jax
import jax.numpy as jnp
from jax import lax

LAYERS = 8
HIDDEN = 256
VOCAB_SIZE = 32000
SEQ_LEN = 16
BATCH_DEV = 32
GROUP_SIZE = 32
BATCH = BATCH_DEV * GROUP_SIZE


def setup_inputs(seed: int = 0) -> dict:
    key_list = jax.random.split(jax.random.key(seed), 5)
    x_in = jax.random.normal(key_list[0], (BATCH, SEQ_LEN, HIDDEN), jnp.float32).astype(jnp.bfloat16)
    targets = jax.random.randint(key_list[1], (BATCH, SEQ_LEN), 0, VOCAB_SIZE, jnp.int32)
    w_lstm = jax.random.normal(key_list[2], (LAYERS, 2 * HIDDEN, 4 * HIDDEN), jnp.float32) * (2 * HIDDEN) ** -0.5
    forget_shift = jnp.concatenate([jnp.zeros((HIDDEN,), jnp.float32), jnp.ones((HIDDEN,), jnp.float32), jnp.zeros((2 * HIDDEN,), jnp.float32)])
    b_lstm = 0.5 * jax.random.normal(key_list[3], (LAYERS, 4 * HIDDEN), jnp.float32) + forget_shift
    w_vocab = jax.random.normal(key_list[4], (HIDDEN, VOCAB_SIZE), jnp.float32) * HIDDEN ** -0.5
    return {'x_in': x_in, 'targets': targets, 'w_lstm': w_lstm.astype(jnp.bfloat16), 'b_lstm': b_lstm, 'w_vocab': w_vocab.astype(jnp.bfloat16)}


def lstm_forward(seq_in, w_layer, b_layer):
    seq_len, num_rows, hidden = seq_in.shape
    w_rec = w_layer[hidden:]
    z_in = jnp.dot(seq_in.reshape(seq_len * num_rows, hidden), w_layer[:hidden], preferred_element_type=jnp.float32)
    z_in = z_in.reshape(seq_len, num_rows, 4 * hidden) + b_layer

    def time_step(carry_in, z_step):
        h_low, c_prev = carry_in
        z_all = z_step + jnp.dot(h_low, w_rec, preferred_element_type=jnp.float32)
        gate_i = jax.nn.sigmoid(z_all[:, :hidden])
        gate_f = jax.nn.sigmoid(z_all[:, hidden:2 * hidden])
        gate_g = jnp.tanh(z_all[:, 2 * hidden:3 * hidden])
        gate_o = jax.nn.sigmoid(z_all[:, 3 * hidden:])
        c_new = gate_f * c_prev + gate_i * gate_g
        tanh_c = jnp.tanh(c_new)
        h_new = gate_o * tanh_c
        gate_all = jnp.concatenate([gate_i, gate_f, gate_g, gate_o], axis=-1)
        return (h_new.astype(jnp.bfloat16), c_new), (h_new, h_low, gate_all, c_prev, tanh_c)

    init_state = (jnp.zeros((num_rows, hidden), jnp.bfloat16), jnp.zeros((num_rows, hidden), jnp.float32))
    final_state, stored = lax.scan(time_step, init_state, z_in)
    h_seq, h_prev, gate_seq, c_prev_seq, tanh_seq = stored
    u_seq = jnp.concatenate([seq_in, h_prev], axis=-1)
    next_in = (seq_in.astype(jnp.float32) + h_seq).astype(jnp.bfloat16)
    return next_in, (u_seq, gate_seq, c_prev_seq, tanh_seq)


def lstm_backward(d_out, stored, w_layer):
    u_seq, gate_seq, c_prev_seq, tanh_seq = stored
    seq_len, num_rows, hidden = d_out.shape
    w_rec_t = w_layer[hidden:].T

    def time_step(carry_in, step_in):
        dh_rec, dc_next = carry_in
        d_ext, gate_all, cell_prev, tanh_c = step_in
        gate_i = gate_all[:, :hidden]
        gate_f = gate_all[:, hidden:2 * hidden]
        gate_g = gate_all[:, 2 * hidden:3 * hidden]
        gate_o = gate_all[:, 3 * hidden:]
        grad_h = d_ext + dh_rec
        dc_tot = dc_next + grad_h * gate_o * (1.0 - tanh_c * tanh_c)
        dz_all = jnp.concatenate([
            dc_tot * gate_g * gate_i * (1.0 - gate_i),
            dc_tot * cell_prev * gate_f * (1.0 - gate_f),
            dc_tot * gate_i * (1.0 - gate_g * gate_g),
            grad_h * tanh_c * gate_o * (1.0 - gate_o)], axis=-1)
        dz_low = dz_all.astype(jnp.bfloat16)
        dh_prev = jnp.dot(dz_low, w_rec_t, preferred_element_type=jnp.float32)
        return (dh_prev, dc_tot * gate_f), (dz_low, jnp.sum(dz_all, axis=0))

    init_state = (jnp.zeros((num_rows, hidden), jnp.float32), jnp.zeros((num_rows, hidden), jnp.float32))
    final_state, outs_seq = lax.scan(time_step, init_state, (d_out, gate_seq, c_prev_seq, tanh_seq), reverse=True)
    dz_seq, db_steps = outs_seq
    dz_flat = dz_seq.reshape(seq_len * num_rows, 4 * hidden)
    dw_layer = jnp.dot(u_seq.reshape(seq_len * num_rows, 2 * hidden).T, dz_flat, preferred_element_type=jnp.float32)
    dx_part = jnp.dot(dz_flat, w_layer[:hidden].T, preferred_element_type=jnp.float32)
    d_in = d_out + dx_part.reshape(seq_len, num_rows, hidden)
    return dw_layer, jnp.sum(db_steps, axis=0), d_in


def head_backward(top_in, tgt_seq, w_vocab):
    seq_len, num_rows, hidden = top_in.shape
    top_flat = top_in.reshape(seq_len * num_rows, hidden)
    logits = jnp.dot(top_flat, w_vocab, preferred_element_type=jnp.float32)
    prob_all = jax.nn.softmax(logits, axis=-1)
    is_target = jnp.arange(w_vocab.shape[1])[None, :] == tgt_seq.reshape(-1)[:, None]
    d_logits = jnp.where(is_target, prob_all - 1.0, prob_all).astype(jnp.bfloat16)
    dw_vocab = jnp.dot(top_flat.T, d_logits, preferred_element_type=jnp.float32)
    d_top = jnp.dot(d_logits, w_vocab.T, preferred_element_type=jnp.float32)
    return d_top.reshape(seq_len, num_rows, hidden), dw_vocab


def shard_grads(x_rows, tgt_rows, w_lstm, b_lstm, w_vocab):
    num_layers = w_lstm.shape[0]
    seq_in = jnp.swapaxes(x_rows, 0, 1)
    saved_acts = []
    for layer_idx in range(num_layers):
        seq_in, stored = lstm_forward(seq_in, w_lstm[layer_idx], b_lstm[layer_idx])
        saved_acts.append(stored)
    d_seq, dw_vocab = head_backward(seq_in, jnp.swapaxes(tgt_rows, 0, 1), w_vocab)
    dw_list = []
    db_list = []
    for layer_idx in reversed(range(num_layers)):
        dw_layer, db_layer, d_seq = lstm_backward(d_seq, saved_acts[layer_idx], w_lstm[layer_idx])
        dw_list.insert(0, dw_layer)
        db_list.insert(0, db_layer)
    return jnp.stack(dw_list), jnp.stack(db_list), dw_vocab, jnp.swapaxes(d_seq, 0, 1)


def reference(x_in, targets, w_lstm, b_lstm, w_vocab):
    x_groups = x_in.reshape(GROUP_SIZE, BATCH_DEV, SEQ_LEN, HIDDEN)
    tgt_groups = targets.reshape(GROUP_SIZE, BATCH_DEV, SEQ_LEN)

    def shard_step(totals, group_in):
        dw_part, db_part, dv_part, dx_part = shard_grads(group_in[0], group_in[1], w_lstm, b_lstm, w_vocab)
        return (totals[0] + dw_part, totals[1] + db_part, totals[2] + dv_part), dx_part

    init_totals = (jnp.zeros(w_lstm.shape, jnp.float32), jnp.zeros(b_lstm.shape, jnp.float32), jnp.zeros(w_vocab.shape, jnp.float32))
    totals, dx_groups = lax.scan(shard_step, init_totals, (x_groups, tgt_groups))
    return totals[0], totals[1], totals[2], dx_groups.reshape(BATCH, SEQ_LEN, HIDDEN)
```

```python
import functools

import jax
import jax.numpy as jnp
from jax import lax
from jax.experimental import pallas as pl
from jax.experimental.pallas import tpu as pltpu
from jax.sharding import PartitionSpec as P

F32 = jnp.float32
BF16 = jnp.bfloat16
VMEM_CAP = 60 * 1024 * 1024
VOCAB_BLK = 1280
SHARD = 1024


def mm(lhs, rhs, dims=((1,), (0,))):
    return lax.dot_general(lhs, rhs, (dims, ((), ())), preferred_element_type=F32)


def sig(val):
    return 0.5 * jnp.tanh(0.5 * val) + 0.5


def fwd_kernel(steps, rows, hid, x_ref, w_ref, b_ref, u_ref, coef_ref, top_ref, xs, zin):
    layer = pl.program_id(0)

    @pl.when(layer == 0)
    def _():
        xs[...] = x_ref[...]

    x_val = xs[...]
    u_ref[0, :, :hid] = x_val
    zin[...] = mm(x_val, w_ref[0, :hid, :]) + b_ref[0]
    h_low = jnp.zeros((rows, hid), BF16)
    cell = jnp.zeros((rows, hid), F32)
    for step in range(steps):
        ts = pl.ds(step * rows, rows)
        u_ref[0, ts, hid:] = h_low
        z_all = zin[ts, :]
        if step:
            z_all = z_all + mm(h_low, w_ref[0, hid:, :])
        gi = sig(z_all[:, :hid])
        gf = sig(z_all[:, hid:2 * hid])
        gg = jnp.tanh(z_all[:, 2 * hid:3 * hid])
        go = sig(z_all[:, 3 * hid:])
        c_new = gf * cell + gi * gg
        tc = jnp.tanh(c_new)
        h_new = go * tc
        h_low = h_new.astype(BF16)
        coef_ref[0, ts, 0 * hid:1 * hid] = gg * gi * (1.0 - gi)
        coef_ref[0, ts, 1 * hid:2 * hid] = cell * gf * (1.0 - gf)
        coef_ref[0, ts, 2 * hid:3 * hid] = gi * (1.0 - gg * gg)
        coef_ref[0, ts, 3 * hid:4 * hid] = tc * go * (1.0 - go)
        coef_ref[0, ts, 4 * hid:5 * hid] = go * (1.0 - tc * tc)
        coef_ref[0, ts, 5 * hid:6 * hid] = gf
        cell = c_new
        xs[ts, :] = (xs[ts, :].astype(F32) + h_new).astype(BF16)

    @pl.when(layer == pl.num_programs(0) - 1)
    def _():
        top_ref[...] = xs[...]


def run_fwd(x_tok, w_lstm, b_lstm, steps, rows):
    layers, _, wide = w_lstm.shape
    hid = wide // 4
    tok = steps * rows
    return pl.pallas_call(
        functools.partial(fwd_kernel, steps, rows, hid),
        grid=(layers,),
        in_specs=[
            pl.BlockSpec((tok, hid), lambda i: (0, 0)),
            pl.BlockSpec((1, 2 * hid, wide), lambda i: (i, 0, 0)),
            pl.BlockSpec((1, 1, wide), lambda i: (i, 0, 0)),
        ],
        out_specs=[
            pl.BlockSpec((1, tok, 2 * hid), lambda i: (i, 0, 0)),
            pl.BlockSpec((1, tok, 6 * hid), lambda i: (i, 0, 0)),
            pl.BlockSpec((tok, hid), lambda i: (0, 0)),
        ],
        out_shape=[
            jax.ShapeDtypeStruct((layers, tok, 2 * hid), BF16),
            jax.ShapeDtypeStruct((layers, tok, 6 * hid), F32),
            jax.ShapeDtypeStruct((tok, hid), BF16),
        ],
        scratch_shapes=[pltpu.VMEM((tok, hid), BF16), pltpu.VMEM((tok, wide), F32)],
        compiler_params=pltpu.CompilerParams(vmem_limit_bytes=VMEM_CAP),
        name='lstm_fwd',
        cost_estimate=pl.CostEstimate(flops=70_000_000_000, bytes_accessed=40_000_000, transcendentals=0),
    )(x_tok, w_lstm, b_lstm.reshape(layers, 1, wide))


def head_kernel(blk, x_ref, w_ref, tgt_ref, dtop_ref, stat_ref, m_s, s_s, acc):
    phase, blk_id = pl.program_id(0), pl.program_id(1)
    tok = x_ref.shape[0]
    lanes = 128
    parts = blk // lanes
    chunk = 128

    @pl.when((phase == 0) & (blk_id == 0))
    def _():
        m_s[...] = jnp.full(m_s.shape, -jnp.inf, F32)
        s_s[...] = jnp.zeros(s_s.shape, F32)
        acc[...] = jnp.zeros(acc.shape, F32)

    @pl.when(phase == 0)
    def _():
        for r0 in range(0, tok, chunk):
            rs = pl.ds(r0, chunk)
            logits = mm(x_ref[rs, :], w_ref[...])
            cols = [logits[:, k * lanes:(k + 1) * lanes] for k in range(parts)]
            m_old = m_s[rs, :]
            m_new = functools.reduce(jnp.maximum, cols, m_old)
            tot = s_s[rs, :] * jnp.exp(m_old - m_new)
            for col in cols:
                tot = tot + jnp.exp(col - m_new)
            m_s[rs, :] = m_new
            s_s[rs, :] = tot

    @pl.when((phase == 0) & (blk_id == pl.num_programs(1) - 1))
    def _():
        m_lane = m_s[...]
        m_row = jnp.max(m_lane, axis=1, keepdims=True)
        s_row = jnp.sum(s_s[...] * jnp.exp(m_lane - m_row), axis=1, keepdims=True)
        m_rep = jnp.broadcast_to(m_row, m_lane.shape)
        r_rep = jnp.broadcast_to(1.0 / s_row, m_lane.shape)
        m_s[...] = m_rep
        s_s[...] = r_rep
        stat_ref[0:1, :] = m_rep.T[0:1, :]
        stat_ref[1:2, :] = r_rep.T[0:1, :]
        stat_ref[2:3, :] = tgt_ref[...].astype(F32).T[0:1, :]
        stat_ref[3:8, :] = jnp.zeros((5, tok), F32)

    @pl.when(phase == 1)
    def _():
        lane_id = lax.broadcasted_iota(jnp.int32, (chunk, lanes), 1) + blk_id * blk
        for r0 in range(0, tok, chunk):
            rs = pl.ds(r0, chunk)
            logits = mm(x_ref[rs, :], w_ref[...])
            m_row, r_row = m_s[rs, :], s_s[rs, :]
            off = tgt_ref[rs, :] - lane_id
            pieces = []
            for k in range(parts):
                prob = jnp.exp(logits[:, k * lanes:(k + 1) * lanes] - m_row) * r_row
                pieces.append(jnp.where(off == k * lanes, prob - 1.0, prob).astype(BF16))
            grad = jnp.concatenate(pieces, axis=1)
            acc[rs, :] += mm(grad, w_ref[...], ((1,), (1,)))

    @pl.when((phase == 1) & (blk_id == pl.num_programs(1) - 1))
    def _():
        dtop_ref[...] = acc[...]


def run_head(x_top, w_vocab, tgt_rep):
    tok, hid = x_top.shape
    vocab = w_vocab.shape[1]
    return pl.pallas_call(
        functools.partial(head_kernel, VOCAB_BLK),
        grid=(2, vocab // VOCAB_BLK),
        in_specs=[
            pl.BlockSpec((tok, hid), lambda p, j: (0, 0)),
            pl.BlockSpec((hid, VOCAB_BLK), lambda p, j: (0, j)),
            pl.BlockSpec((tok, 128), lambda p, j: (0, 0)),
        ],
        out_specs=[
            pl.BlockSpec((tok, hid), lambda p, j: (0, 0)),
            pl.BlockSpec((8, tok), lambda p, j: (0, 0)),
        ],
        out_shape=[jax.ShapeDtypeStruct((tok, hid), F32), jax.ShapeDtypeStruct((8, tok), F32)],
        scratch_shapes=[pltpu.VMEM((tok, 128), F32), pltpu.VMEM((tok, 128), F32), pltpu.VMEM((tok, hid), F32)],
        compiler_params=pltpu.CompilerParams(vmem_limit_bytes=VMEM_CAP),
        name='head',
        cost_estimate=pl.CostEstimate(flops=70_000_000_000, bytes_accessed=33_000_000, transcendentals=0),
    )(x_top, w_vocab, tgt_rep)


def vocab_kernel(start_ref, x_ref, stat_ref, w_ref, dw_ref, wt, acc):
    blk_id = pl.program_id(0)
    tok = x_ref.shape[0]
    shard = w_ref.shape[1]
    per = stat_ref.shape[0]
    chunk = 256

    @pl.when(blk_id == 0)
    def _():
        wt[...] = w_ref[...].T
        acc[...] = jnp.zeros(acc.shape, F32)

    stats = [jnp.concatenate([stat_ref[p, r:r + 1, :] for p in range(per)], axis=1) for r in range(3)]
    m_row, r_row = stats[0], stats[1]
    tgt = stats[2].astype(jnp.int32) - start_ref[0]
    x_val = x_ref[...]
    for r0 in range(0, shard, chunk):
        rs = pl.ds(r0, chunk)
        logits = mm(wt[rs, :], x_val, ((1,), (1,)))
        prob = jnp.exp(logits - m_row) * r_row
        ids = lax.broadcasted_iota(jnp.int32, (chunk, tok), 0) + r0
        grad = jnp.where(ids == tgt, prob - 1.0, prob).astype(BF16)
        acc[rs, :] += mm(grad, x_val)

    @pl.when(blk_id == pl.num_programs(0) - 1)
    def _():
        dw_ref[...] = acc[...].T


def run_vocab(start, x_all, stat_all, w_shard):
    tok, hid = x_all.shape
    ndev, _, per_dev = stat_all.shape
    per = 2
    shard = w_shard.shape[1]
    return pl.pallas_call(
        vocab_kernel,
        grid=(ndev // per,),
        in_specs=[
            pl.BlockSpec(memory_space=pltpu.SMEM),
            pl.BlockSpec((per * per_dev, hid), lambda i: (i, 0)),
            pl.BlockSpec((per, 8, per_dev), lambda i: (i, 0, 0)),
            pl.BlockSpec((hid, shard), lambda i: (0, 0)),
        ],
        out_specs=pl.BlockSpec((hid, shard), lambda i: (0, 0)),
        out_shape=jax.ShapeDtypeStruct((hid, shard), F32),
        scratch_shapes=[pltpu.VMEM((shard, hid), BF16), pltpu.VMEM((shard, hid), F32)],
        compiler_params=pltpu.CompilerParams(vmem_limit_bytes=VMEM_CAP),
        name='dw_vocab',
        cost_estimate=pl.CostEstimate(flops=40_000_000_000, bytes_accessed=12_000_000, transcendentals=0),
    )(start, x_all, stat_all, w_shard)


def bwd_kernel(steps, rows, hid, d_ref, u_ref, coef_ref, w_ref, dw_ref, db_ref, dx_ref, dx, dz_s, wrt, dbp):
    layer = pl.program_id(0)

    @pl.when(layer == 0)
    def _():
        dx[...] = d_ref[...]

    wrt[...] = w_ref[0, hid:, :].T
    dbp[...] = jnp.zeros(dbp.shape, F32)
    e_rec = jnp.zeros((rows, hid), F32)
    dc_rec = jnp.zeros((rows, hid), F32)
    for step in reversed(range(steps)):
        ts = pl.ds(step * rows, rows)
        err = dx[ts, :] + e_rec
        dct = dc_rec + err * coef_ref[0, ts, 4 * hid:5 * hid]
        e_rec = jnp.zeros((rows, hid), F32)
        for gate in range(4):
            cols = pl.ds(gate * hid, hid)
            dz = (err if gate == 3 else dct) * coef_ref[0, ts, gate * hid:(gate + 1) * hid]
            low = dz.astype(BF16)
            dz_s[ts, cols] = low
            if step:
                e_rec = e_rec + mm(low, wrt[cols, :])
            part = dz[0:8]
            for k in range(8, rows, 8):
                part = part + dz[k:k + 8]
            dbp[:, cols] += part
        dc_rec = dct * coef_ref[0, ts, 5 * hid:6 * hid]
    db_ref[0] = jnp.sum(dbp[...], axis=0, keepdims=True)
    dz_all = dz_s[...]
    dw_ref[0] = mm(u_ref[0], dz_all, ((0,), (0,)))
    dx[...] += mm(dz_all, w_ref[0, :hid, :], ((1,), (1,)))

    @pl.when(layer == pl.num_programs(0) - 1)
    def _():
        dx_ref[...] = dx[...]


def run_bwd(d_top, u_all, coef, w_lstm, steps, rows):
    layers, _, wide = w_lstm.shape
    hid = wide // 4
    tok = steps * rows
    last = layers - 1
    return pl.pallas_call(
        functools.partial(bwd_kernel, steps, rows, hid),
        grid=(layers,),
        in_specs=[
            pl.BlockSpec((tok, hid), lambda i: (0, 0)),
            pl.BlockSpec((1, tok, 2 * hid), lambda i: (last - i, 0, 0)),
            pl.BlockSpec((1, tok, 6 * hid), lambda i: (last - i, 0, 0)),
            pl.BlockSpec((1, 2 * hid, wide), lambda i: (last - i, 0, 0)),
        ],
        out_specs=[
            pl.BlockSpec((1, 2 * hid, wide), lambda i: (last - i, 0, 0)),
            pl.BlockSpec((1, 1, wide), lambda i: (last - i, 0, 0)),
            pl.BlockSpec((tok, hid), lambda i: (0, 0)),
        ],
        out_shape=[
            jax.ShapeDtypeStruct((layers, 2 * hid, wide), F32),
            jax.ShapeDtypeStruct((layers, 1, wide), F32),
            jax.ShapeDtypeStruct((tok, hid), F32),
        ],
        scratch_shapes=[
            pltpu.VMEM((tok, hid), F32),
            pltpu.VMEM((tok, wide), BF16),
            pltpu.VMEM((wide, hid), BF16),
            pltpu.VMEM((8, wide), F32),
        ],
        compiler_params=pltpu.CompilerParams(vmem_limit_bytes=VMEM_CAP),
        name='lstm_bwd',
        cost_estimate=pl.CostEstimate(flops=80_000_000_000, bytes_accessed=60_000_000, transcendentals=0),
    )(d_top, u_all, coef, w_lstm)


def solution(mesh):
    ndev = mesh.shape['data']

    def local_grads(x_rows, tgt_rows, w_lstm, b_lstm, w_vocab):
        rows, steps, hid = x_rows.shape
        tok = rows * steps
        vocab = w_vocab.shape[1]
        me = lax.axis_index('data')
        x_tok = jnp.swapaxes(x_rows, 0, 1).reshape(tok, hid)
        tgt_rep = jnp.broadcast_to(jnp.swapaxes(tgt_rows, 0, 1).reshape(tok, 1), (tok, 128))
        start = jnp.minimum(me * SHARD, vocab - SHARD)
        w_shard = lax.dynamic_slice(w_vocab, (0, start), (hid, SHARD))

        u_all, coef, x_top = run_fwd(x_tok, w_lstm, b_lstm, steps, rows)
        x_all = lax.all_gather(x_top, 'data', axis=0, tiled=True)
        d_top, stat = run_head(x_top, w_vocab, tgt_rep)
        stat_all = lax.all_gather(stat, 'data', axis=0)
        dwv = run_vocab(start.reshape(1), x_all, stat_all, w_shard)
        dwv_all = lax.all_gather(dwv, 'data', axis=0)
        tail = vocab - (ndev - 1) * SHARD
        main = jnp.swapaxes(dwv_all[:ndev - 1], 0, 1).reshape(hid, (ndev - 1) * SHARD)
        dw_vocab = jnp.concatenate([main, dwv_all[ndev - 1][:, SHARD - tail:]], axis=1)
        dw, db, dx = run_bwd(d_top, u_all, coef, w_lstm, steps, rows)
        dw, db = lax.psum((dw, db), 'data')
        dx_rows = jnp.swapaxes(dx.reshape(steps, rows, hid), 0, 1)
        return dw, db.reshape(b_lstm.shape), dw_vocab, dx_rows

    return jax.shard_map(local_grads, mesh=mesh, in_specs=(P('data'), P('data'), P(), P(), P()), out_specs=(P(), P(), P(), P('data')), check_vma=False)
```

```python
import functools

import jax
import jax.numpy as jnp
from jax import lax
from jax.experimental import pallas as pl
from jax.experimental.pallas import tpu as pltpu
from jax.sharding import PartitionSpec as P

F32 = jnp.float32
BF16 = jnp.bfloat16
VMEM_CAP = 60 * 1024 * 1024
VOCAB_BLK = 1280
SHARD = 1024
VOCAB = 32000
LANES = 128
SUBL = 8
NSEM = 192
XPARTS = 1
XEARLY = 7


def mm(lhs, rhs, dims=((1,), (0,))):
    return lax.dot_general(lhs, rhs, (dims, ((), ())), preferred_element_type=F32)


def sig(val):
    return 0.5 * jnp.tanh(0.5 * val) + 0.5


MESH_ID = pl.DeviceIdType.MESH
SIDES = ((0, 1), (1, 0))
QUAD = ((0, 0), (0, 1), (1, 0), (1, 1))
FAR = (1, 2, 3)
HERE = (0, 0, 0, False)
LINE = (0, 1, 2, 3)


class Place:
    def __init__(self, me):
        self.me = me
        half, quarter = lax.div(me, 2), lax.div(me, 4)
        self.core, self.x, self.y, self.z = (
            lax.rem(me, 2), lax.rem(half, 2), lax.rem(quarter, 2), lax.div(me, 8))
        self.zs = [self.z, self.z + 1 - 2 * lax.rem(self.z, 2), lax.rem(self.z + 2, 4), 3 - self.z]
        self.at = {}
        for k in LINE:
            for fy, fx in QUAD:
                for other in (False, True):
                    y = 1 - self.y if fy else self.y
                    x = 1 - self.x if fx else self.x
                    c = 1 - self.core if other else self.core
                    self.at[k, fy, fx, other] = (self.zs[k], y, x, c)
        self.devs = {key: ((z * 2 + y) * 2 + x) * 2 + c for key, (z, y, x, c) in self.at.items()}
        self.partner = self.dev(0, 0, 0, True)

    def dev(self, k, fy, fx, other=False):
        return self.devs[k, fy, fx, other]

    def barrier(self):
        peers = [self.dev(k, 0, 0) for k in FAR] + [self.dev(0, *side) for side in SIDES] + [self.partner]
        sem = pltpu.get_barrier_semaphore()
        for peer in peers:
            pl.semaphore_signal(sem, device_id=(peer,), device_id_type=MESH_ID)
        pl.semaphore_wait(sem, len(peers))


class Link:
    def __init__(self, send, recv):
        self.send, self.recv, self.keys = send, recv, {}

    def copy(self, key, src, dst, peer):
        at = self.keys.setdefault(key, len(self.keys))
        return pltpu.make_async_remote_copy(
            src_ref=src, dst_ref=dst, send_sem=self.send.at[at], recv_sem=self.recv.at[at],
            device_id=(peer,), device_id_type=MESH_ID)


class Gather:
    def __init__(self, place, link, name, own, slot, half):
        self.p, self.link, self.name, self.own, self.slot, self.half = place, link, name, own, slot, half
        self.sent = []

    def _send(self, key, at, to, other=False, half=None):
        at = at + (False,)

        def make():
            if half is None:
                dst = self.slot(at)
                src = dst if any(at) else self.own
            else:
                src = dst = self.half(at, half)
            return self.link.copy((self.name,) + key, src, dst, self.p.dev(*to, other))

        self.sent.append(make)
        make().start()

    def _arrive(self, key, at, other=False, half=None):
        at = at + (other,)
        ref = self.slot(at) if half is None else self.half(at, half)
        self.link.copy((self.name,) + key, ref, ref, self.p.partner).wait_recv()

    def _pair(self, *at):
        self._send(('pair',) + at, at, LINE[:1] + QUAD[0], True)

    def _line(self, k):
        for side in SIDES:
            self._send(('line', k) + side, (k, 0, 0), (0,) + side)

    def _far(self):
        for k in FAR:
            self._send(('far', k), LINE[:1] + QUAD[0], (k,) + QUAD[0])

    def start(self):
        self._line(0)
        self._far()
        self._pair(0, 0, 0)

    def take_far(self, k):
        self._arrive(('far', k), (k,) + QUAD[0])
        self._line(k)
        self._pair(k, *QUAD[0])

    def take_line(self, k):
        for h, side in enumerate(SIDES):
            self._arrive(('line', k) + side, (k,) + side)
            self._send(('diag', k, h), (k,) + side, (0,) + SIDES[1 - h], half=h)
            self._pair(k, *side)

    def take_diag(self, k):
        for h in range(2):
            self._arrive(('diag', k, h), (k,) + QUAD[3], half=h)
        self._pair(k, *QUAD[3])

    def finish(self):
        for k in LINE:
            for side in QUAD:
                self._arrive(('pair', k) + side, (k,) + side, True)
        for make in self.sent:
            make().wait_send()

    def steps(self):
        far = [functools.partial(self.take_far, k) for k in LINE]
        line = [functools.partial(self.take_line, k) for k in LINE]
        diag = [functools.partial(self.take_diag, k) for k in LINE]
        return [far[1], line[0], far[2], line[1], far[3], diag[0], line[2], diag[1], line[3]] + diag[2:]


def fwd_kernel(steps, rows, hid, x_ref, w_ref, b_ref, u_ref, coef_ref, top_ref, xs, zin):
    layer = pl.program_id(0)

    @pl.when(layer == 0)
    def _():
        xs[...] = x_ref[...]

    x_val = xs[...]
    u_ref[0, :, :hid] = x_val
    zin[...] = mm(x_val, w_ref[0, :hid, :]) + b_ref[pl.ds(layer, 1), :]
    h_low = jnp.zeros((rows, hid), BF16)
    cell = jnp.zeros((rows, hid), F32)
    for step in range(steps):
        ts = pl.ds(step * rows, rows)
        u_ref[0, ts, hid:] = h_low
        z_all = zin[ts, :]
        if step:
            z_all = z_all + mm(h_low, w_ref[0, hid:, :])
        gi = sig(z_all[:, :hid])
        gf = sig(z_all[:, hid:2 * hid])
        gg = jnp.tanh(z_all[:, 2 * hid:3 * hid])
        go = sig(z_all[:, 3 * hid:])
        c_new = gf * cell + gi * gg
        tc = jnp.tanh(c_new)
        h_new = go * tc
        h_low = h_new.astype(BF16)
        coefs = (gg * gi * (1.0 - gi), cell * gf * (1.0 - gf), gi * (1.0 - gg * gg), tc * go * (1.0 - go),
                 go * (1.0 - tc * tc), gf)
        for at, val in enumerate(coefs):
            coef_ref[0, ts, at * hid:(at + 1) * hid] = val
        cell = c_new
        xs[ts, :] = (xs[ts, :].astype(F32) + h_new).astype(BF16)

    @pl.when(layer == pl.num_programs(0) - 1)
    def _():
        top_ref[...] = xs[...]


def run_fwd(x_tok, w_lstm, b_lstm, steps, rows):
    layers, _, wide = w_lstm.shape
    hid = wide // 4
    tok = steps * rows
    return pl.pallas_call(
        functools.partial(fwd_kernel, steps, rows, hid),
        grid=(layers,),
        in_specs=[
            pl.BlockSpec((tok, hid), lambda i: (0, 0)),
            pl.BlockSpec((1, 2 * hid, wide), lambda i: (i, 0, 0)),
            pl.BlockSpec((layers, wide), lambda i: (0, 0)),
        ],
        out_specs=[
            pl.BlockSpec((1, tok, 2 * hid), lambda i: (i, 0, 0)),
            pl.BlockSpec((1, tok, 6 * hid), lambda i: (i, 0, 0)),
            pl.BlockSpec((tok, hid), lambda i: (0, 0)),
        ],
        out_shape=[
            jax.ShapeDtypeStruct((layers, tok, 2 * hid), BF16),
            jax.ShapeDtypeStruct((layers, tok, 6 * hid), F32),
            jax.ShapeDtypeStruct((tok, hid), BF16),
        ],
        scratch_shapes=[pltpu.VMEM((tok, hid), BF16), pltpu.VMEM((tok, wide), F32)],
        compiler_params=pltpu.CompilerParams(vmem_limit_bytes=VMEM_CAP),
        name='lstm_fwd',
        cost_estimate=pl.CostEstimate(flops=70_000_000_000, bytes_accessed=40_000_000, transcendentals=0),
    )(x_tok, w_lstm, b_lstm)


def head_kernel(blk, x_ref, w_ref, tgt_ref, xall_ref, sall_ref, m_ref, r_ref, m_s, s_s, stat_s, ssem, rsem, lsem):
    blk_id = pl.program_id(0)
    last = pl.num_programs(0) - 1
    tok = x_ref.shape[0]
    place = Place(lax.axis_index('data'))
    link = Link(ssem, rsem)
    mid = tok // 2

    def chunk_at(part):
        num = tok // XPARTS
        row = lambda dev, h, n: pl.ds(pl.multiple_of(dev * tok + part * num + h * n, n), n)
        return Gather(place, link, ('x', part), x_ref.at[pl.ds(part * num, num), :],
                      lambda at: xall_ref.at[row(place.devs[at], 0, num), :],
                      lambda at, h: xall_ref.at[row(place.devs[at], h, num // 2), :])

    gats = [chunk_at(part) for part in range(XPARTS)]
    gat_s = Gather(place, link, 's', stat_s, lambda at: sall_ref.at[place.devs[at]],
                   lambda at, h: sall_ref.at[place.devs[at], :, pl.ds(h * mid, mid)])
    loc_x = [pltpu.make_async_copy(g.own, g.slot(HERE), lsem.at[1 + at]) for at, g in enumerate(gats)]
    loc_s = pltpu.make_async_copy(stat_s, gat_s.slot(HERE), lsem.at[0])
    sx, ss = [act for acts in zip(*[g.steps() for g in gats]) for act in acts], gat_s.steps()

    @pl.when(blk_id == 0)
    def _():
        place.barrier()
        for gat, loc in zip(gats, loc_x):
            gat.start()
            loc.start()
        m_s[...] = jnp.full(m_s.shape, -jnp.inf, F32)
        s_s[...] = jnp.zeros(s_s.shape, F32)

    for at, act in zip(range(6, VOCAB // blk - 1), sx[:XEARLY]):
        pl.when(blk_id == at)(act)

    for r0 in range(0, tok, LANES):
        rs = pl.ds(r0, LANES)
        logits = mm(x_ref[rs, :], w_ref[...])
        cols = [logits[:, k:k + LANES] for k in range(0, blk, LANES)]
        m_old = m_s[rs, :]
        m_new = functools.reduce(jnp.maximum, cols, m_old)
        tot = s_s[rs, :] * jnp.exp(m_old - m_new)
        for col in cols:
            tot = tot + jnp.exp(col - m_new)
        m_s[rs, :] = m_new
        s_s[rs, :] = tot

    @pl.when(blk_id == last)
    def _():
        m_lane = m_s[...]
        m_row = jnp.max(m_lane, axis=1, keepdims=True)
        s_row = jnp.sum(s_s[...] * jnp.exp(m_lane - m_row), axis=1, keepdims=True)
        m_rep = jnp.broadcast_to(m_row, m_lane.shape)
        r_rep = jnp.broadcast_to(1.0 / s_row, m_lane.shape)
        m_ref[...] = m_rep
        r_ref[...] = r_rep
        stat_s[...] = jnp.zeros(stat_s.shape, F32)
        for at, val in enumerate((m_rep, r_rep, tgt_ref[...].astype(F32))):
            stat_s[at:at + 1, :] = val.T[:1, :]
        gat_s.start()
        loc_s.start()
        for at in range(len(ss)):
            for act in sx[XEARLY + at:XEARLY + at + 1] + ss[at:at + 1]:
                act()
        for act in sx[XEARLY + len(ss):]:
            act()
        for gat in gats + [gat_s]:
            gat.finish()
        for loc in loc_x + [loc_s]:
            loc.wait()


def run_head(x_top, w_vocab, tgt_rep, ndev):
    tok, hid = x_top.shape
    full = pl.BlockSpec(memory_space=pltpu.VMEM)
    anyw = pl.BlockSpec(memory_space=pl.ANY)
    stat = jax.ShapeDtypeStruct((tok, LANES), F32)
    same = pl.BlockSpec((tok, LANES), lambda j: (0, 0))
    return pl.pallas_call(
        functools.partial(head_kernel, VOCAB_BLK),
        grid=(VOCAB // VOCAB_BLK,),
        in_specs=[full, pl.BlockSpec((hid, VOCAB_BLK), lambda j: (0, j)), full],
        out_specs=[anyw, anyw, same, same],
        out_shape=[
            jax.ShapeDtypeStruct((ndev * tok, hid), BF16),
            jax.ShapeDtypeStruct((ndev, SUBL, tok), F32), stat, stat,
        ],
        scratch_shapes=[
            pltpu.VMEM((tok, LANES), F32), pltpu.VMEM((tok, LANES), F32), pltpu.VMEM((SUBL, tok), F32),
            pltpu.SemaphoreType.DMA((LANES,)), pltpu.SemaphoreType.DMA((LANES,)), pltpu.SemaphoreType.DMA((1 + XPARTS,)),
        ],
        compiler_params=pltpu.CompilerParams(vmem_limit_bytes=VMEM_CAP, collective_id=1, has_side_effects=True),
        name='head',
        cost_estimate=pl.CostEstimate(flops=10**10, bytes_accessed=10**7, transcendentals=0),
    )(x_top, w_vocab, tgt_rep)


GROUP = 4
SPLIT = 2
WID = SHARD // SPLIT
TOK_BLK = 1024


class Reduce:
    def __init__(self, place, link, grp, buf, boxes):
        self.p, self.link, self.grp, self.buf, self.boxes = place, link, grp, buf, boxes
        self.first = grp * GROUP
        self.lay = pl.ds(self.first, GROUP)
        p = place
        xdev, ydev = p.dev(0, *SIDES[0]), p.dev(0, *SIDES[1])
        pick = lambda one, two: (1 - p.core) * one + p.core * two
        self.peers = [p.partner, pick(xdev, ydev), pick(ydev, xdev)]
        self.give, self.keep, self.size, base = [], [], [], 0
        for at, bit in enumerate((p.core, pick(p.x, p.y), pick(p.y, p.x))):
            size = buf.shape[1] >> (at + 1)
            self.size.append(size)
            self.give.append(base + (1 - bit) * size)
            base = base + bit * size
            self.keep.append(base)
        self.unit = size // len(LINE)
        self.base = base
        self.sent = []

    def _rows(self, start, num):
        return pl.ds(pl.multiple_of(start, num), num)

    def _copies(self, at):
        if at < len(self.size):
            src = self.buf.at[self.lay, self._rows(self.give[at], self.size[at]), :]
            return [self.link.copy(('sum', self.grp, at), src, self.boxes[at].at[self.lay], self.peers[at])]
        out = []
        for k in FAR:
            src = self.buf.at[self.lay, self._rows(self.base + self.p.zs[k] * self.unit, self.unit), :]
            dst = self.boxes[at].at[k - 1, self.lay]
            out.append(self.link.copy(('sum', self.grp, at, k), src, dst, self.p.dev(k, 0, 0)))
        return out

    def start(self, at=0):
        for copy in self._copies(at):
            copy.start()

    def take(self, at):
        for copy in self._copies(at):
            copy.wait_recv()
        far = at == len(self.size)
        num = self.unit if far else self.size[at]
        rows = self._rows(self.base + self.p.z * num if far else self.keep[at], num)
        for i in range(GROUP):
            lay = self.first + i
            val = self.buf[lay, rows, :]
            for k in FAR if far else FAR[:1]:
                val = val + (self.boxes[at][k - 1, lay] if far else self.boxes[at][lay])
            self.buf[lay, rows, :] = val
        if not far:
            self.start(at + 1)

    def finish(self):
        for at in LINE:
            for copy in self._copies(at):
                copy.wait_send()


def main_kernel(phases, steps, rows, hid, x_ref, stat_ref, wv_ref, wsh_ref, m_ref, r_ref, tgt_ref, xl_ref,
                u_ref, coef_ref, w_ref, dw_ref, db_ref, dx_ref, dv_ref,
                wt, acc, shv, dx, dz_s, wrt, dbp, buf, r0, r1, r2, r3, dbb, dball, gs, gr, ls):
    step_id = pl.program_id(0)
    n_vocab, n_top, n_layers = phases
    t_top = n_vocab
    t_bwd = n_vocab + n_top
    t_last = t_bwd + n_layers - 1
    place = Place(lax.axis_index('data'))
    link = Link(gs, gr)
    ndev = stat_ref.shape[0] * n_vocab // SPLIT
    tail = dball.shape[0] - 1

    def chunk_at(q):
        cols = lambda at: pl.ds(pl.multiple_of(place.devs[at] * SHARD + q * WID, WID), WID)
        return Gather(
            place, link, ('v', q), shv.at[q], lambda at: dv_ref.at[:, cols(at)],
            lambda at, h: dv_ref.at[pl.ds(h * (hid // 2), hid // 2), cols(at)])

    def piece(at):
        z, y, x, c = place.at[at]
        far, near = hid // 2, hid // 4
        return c * hid + ((1 - c) * x + c * y) * far + ((1 - c) * y + c * x) * near + z * (near // 4)

    pieces = {at: piece(at) for at in place.at}

    def group_at(grp):
        lay = pl.ds(grp * GROUP, GROUP)
        unit = hid // 16
        part = lambda at, h, n: pl.ds(pl.multiple_of(pieces[at] + h * n, n), n)
        return Gather(
            place, link, ('w', grp), buf.at[lay, part(HERE, 0, unit), :],
            lambda at: dw_ref.at[lay, part(at, 0, unit), :],
            lambda at, h: dw_ref.at[lay, part(at, h, unit // 2), :])

    gats = [chunk_at(q) for q in range(SPLIT)]
    n_grp = n_layers // GROUP
    reds = [Reduce(place, link, n_grp - 1 - j, buf, (r0, r1, r2, r3)) for j in range(n_grp)]
    outs = [group_at(n_grp - 1 - j) for j in range(n_grp)]
    wide2 = dbb.shape[1] // 2
    gdb = Gather(place, link, 'b', dbb, lambda at: dball.at[place.devs[at]],
                 lambda at, h: dball.at[place.devs[at], :, pl.ds(h * wide2, wide2)])
    own_v = [pltpu.make_async_copy(shv.at[q], gats[q].slot(HERE), ls.at[q]) for q in range(SPLIT)]
    own_w = [pltpu.make_async_copy(outs[g].own, outs[g].slot(HERE), ls.at[SPLIT + g]) for g in range(n_grp)]
    def slot_of(when):
        if when >= t_top:
            when = t_top + (when - t_top) * 5 // SUBL
        return when if when < t_bwd else t_bwd + (when - t_bwd) // 4

    per_chunk = n_vocab // SPLIT
    todo = sorted(
        (per_chunk * (q + 1) + 6 + 9 * n, q, n) for q in range(SPLIT) for n in range(len(gats[q].steps())))
    acts = [(slot_of(when), gats[q].steps()[n]) for when, q, n in todo]

    def emit(j):
        reds[j].take(3)
        outs[j].start()
        own_w[j].start()

    late = []
    for j in range(n_grp):
        ops = [functools.partial(reds[j].take, n) for n in range(3)] + [functools.partial(emit, j)]
        late += [(n, j, op) for n, op in enumerate(ops)]
        late += [(4 + n, j, op) for n, op in enumerate(outs[j].steps())]
    late += [(4 * n_grp + n, n_grp, op) for n, op in enumerate(gdb.steps())]
    late = [op for _, _, op in sorted(late, key=lambda item: item[:2])]

    @pl.when(step_id == 0)
    def _():
        place.barrier()
        wt[...] = wsh_ref[...].T
        dx[...] = jnp.zeros(dx.shape, F32)

    per = n_vocab // SPLIT
    q_now, blk_now = lax.div(step_id, per), lax.rem(step_id, per)

    @pl.when((step_id < t_top) & (blk_now == 0))
    def _():
        acc[...] = jnp.zeros(acc.shape, F32)

    @pl.when(step_id < t_top)
    def _():
        m_row, r_row, tgt = [
            jnp.concatenate([stat_ref[p, r:r + 1, :] for p in range(stat_ref.shape[0])], axis=1) for r in range(3)]
        x_val = x_ref[...]
        logits = mm(wt[pl.ds(pl.multiple_of(q_now * WID, WID), WID), :], x_val, ((1,), (1,)))
        prob = jnp.exp(logits - m_row) * r_row
        ids = lax.broadcasted_iota(jnp.int32, prob.shape, 0) + (place.me * SHARD + q_now * WID)
        dist = ids.astype(F32) - tgt
        hot = jnp.maximum(1.0 - jnp.maximum(dist, -dist), 0.0)
        acc[...] += mm((prob - hot).astype(BF16), x_val)

    for k in range(SPLIT):
        @pl.when(step_id == k * per + per - 1)
        def _(k=k):
            shv[k] = acc[...].T
            gats[k].start()
            own_v[k].start()

    for at, act in acts:
        if at < t_last:
            pl.when(step_id == at)(act)

    @pl.when((step_id >= t_top) & (step_id < t_bwd))
    def _():
        blk = wv_ref.shape[1]
        lane_id = lax.broadcasted_iota(jnp.int32, (LANES, LANES), 1) + (step_id - t_top) * blk

        @pl.loop(0, dx.shape[0] // LANES)
        def _(part):
            rs = pl.ds(pl.multiple_of(part * LANES, LANES), LANES)
            logits = mm(xl_ref[rs, :], wv_ref[...])
            m_row, r_row = m_ref[rs, :], r_ref[rs, :]
            off = tgt_ref[rs, :] - lane_id
            pieces = []
            for k in range(0, blk, LANES):
                prob = jnp.exp(logits[:, k:k + LANES] - m_row) * r_row
                pieces.append(jnp.where(off == k, prob - 1.0, prob).astype(BF16))
            dx[rs, :] += mm(jnp.concatenate(pieces, axis=1), wv_ref[...], ((1,), (1,)))

    @pl.when(step_id >= t_bwd)
    def _():
        lay = t_last - step_id
        wrt[...] = w_ref[0, hid:, :].T
        dbp[...] = jnp.zeros(dbp.shape, F32)
        e_rec = jnp.zeros((rows, hid), F32)
        dc_rec = jnp.zeros((rows, hid), F32)
        for step in reversed(range(steps)):
            ts = pl.ds(step * rows, rows)
            coef = [coef_ref[0, ts, at * hid:(at + 1) * hid] for at in range(6)]
            err = dx[ts, :] + e_rec
            dct = dc_rec + err * coef[4]
            e_rec = jnp.zeros((rows, hid), F32)
            for gate in LINE:
                cols = pl.ds(gate * hid, hid)
                dz = (err if gate == LINE[-1] else dct) * coef[gate]
                low = dz.astype(BF16)
                dz_s[ts, cols] = low
                if step:
                    e_rec = e_rec + mm(low, wrt[cols, :])
                dbp[:, cols] += functools.reduce(jnp.add, [dz[k:k + SUBL] for k in range(0, rows, SUBL)])
            dc_rec = dct * coef[5]
        dbb[pl.ds(lay, 1), :] = jnp.sum(dbp[...], axis=0, keepdims=True)
        dz_all = dz_s[...]
        buf[lay] = mm(u_ref[0], dz_all, ((0,), (0,)))
        dx[...] += mm(dz_all, w_ref[0, :hid, :], ((1,), (1,)))

    for j in range(n_grp):
        pl.when(step_id == t_bwd + GROUP * (j + 1) - 1)(reds[j].start)

    done = 0
    for at, upto in ((4, 1),):
        for act in late[done:upto]:
            pl.when(step_id == t_bwd + at)(act)
        done = upto

    @pl.when(step_id == t_last)
    def _():
        dx_ref[...] = dx[...]
        gdb.start()
        rest = [act for at, act in acts if at >= t_last]
        for at in range(len(late) - done):
            for act in rest[at:at + 1] + late[done + at:done + at + 1]:
                act()
        for act in rest[len(late) - done:]:
            act()
        dball[place.me] = dbb[...]
        gdb.finish()
        total = dball[0]
        for dev in range(1, tail + 1):
            total = total + dball[dev]
        db_ref[...] = total
        for gat in gats + outs:
            gat.finish()
        for q in range(SPLIT):
            own_v[q].wait()
        for copy in own_w:
            copy.wait()
        for red in reds:
            red.finish()


def run_main(x_all, stat_all, w_vocab, w_shard, m_rep, r_rep, tgt_rep, x_last, u_all, coef, w_lstm, steps, rows, ndev):
    layers, _, wide = w_lstm.shape
    hid = wide // 4
    tok = steps * rows
    blocks = ndev * tok // TOK_BLK
    phases = (SPLIT * blocks, VOCAB // VOCAB_BLK, layers)
    t_top = phases[0]
    t_bwd = t_top + phases[1]
    full = pl.BlockSpec(memory_space=pltpu.VMEM)
    anyw = pl.BlockSpec(memory_space=pl.ANY)
    total = sum(phases)
    past = lambda i, at: (i + total - at) // total
    at_tok = lambda i: (1 - past(i, t_top)) * (i % blocks) + past(i, t_top) * (blocks - 1)
    at_voc = lambda i: past(i, t_top) * (1 - past(i, t_bwd)) * (i - t_top) + past(i, t_bwd) * (phases[1] - 1)
    at_lay = lambda i: layers - 1 - past(i, t_bwd) * (i - t_bwd)
    same = lambda shape: pl.BlockSpec(shape, lambda i: (0, 0))
    sem = pltpu.SemaphoreType.DMA
    return pl.pallas_call(
        functools.partial(main_kernel, phases, steps, rows, hid),
        grid=(total,),
        in_specs=[
            pl.BlockSpec((TOK_BLK, hid), lambda i: (at_tok(i), 0)),
            pl.BlockSpec((TOK_BLK // tok, SUBL, tok), lambda i: (at_tok(i), 0, 0)),
            pl.BlockSpec((hid, VOCAB_BLK), lambda i: (0, at_voc(i))),
            full, full, full, full, full,
            pl.BlockSpec((1, tok, 2 * hid), lambda i: (at_lay(i), 0, 0)),
            pl.BlockSpec((1, tok, 6 * hid), lambda i: (at_lay(i), 0, 0)),
            pl.BlockSpec((1, 2 * hid, wide), lambda i: (at_lay(i), 0, 0)),
        ],
        out_specs=[anyw, same((layers, wide)), same((tok, hid)), anyw],
        out_shape=[
            jax.ShapeDtypeStruct((layers, 2 * hid, wide), F32),
            jax.ShapeDtypeStruct((layers, wide), F32),
            jax.ShapeDtypeStruct((tok, hid), F32),
            jax.ShapeDtypeStruct((hid, ndev * SHARD), F32),
        ],
        scratch_shapes=[
            pltpu.VMEM((SHARD, hid), BF16),
            pltpu.VMEM((WID, hid), F32),
            pltpu.VMEM((SPLIT, hid, WID), F32),
            pltpu.VMEM((tok, hid), F32),
            pltpu.VMEM((tok, wide), BF16),
            pltpu.VMEM((wide, hid), BF16),
            pltpu.VMEM((SUBL, wide), F32),
            pltpu.VMEM((layers, 2 * hid, wide), F32),
            pltpu.VMEM((layers, hid, wide), F32),
            pltpu.VMEM((layers, hid // 2, wide), F32),
            pltpu.VMEM((layers, hid // 4, wide), F32),
            pltpu.VMEM((3, layers, hid // 16, wide), F32),
            pltpu.VMEM((layers, wide), F32),
            pltpu.VMEM((ndev, layers, wide), F32),
            sem((NSEM,)), sem((NSEM,)), sem((SPLIT + layers // GROUP,)),
        ],
        compiler_params=pltpu.CompilerParams(vmem_limit_bytes=VMEM_CAP, collective_id=2, has_side_effects=True),
        name='main',
        cost_estimate=pl.CostEstimate(flops=10**10, bytes_accessed=10**7, transcendentals=0),
    )(x_all, stat_all, w_vocab, w_shard, m_rep, r_rep, tgt_rep, x_last, u_all, coef, w_lstm)


def solution(mesh):
    ndev = mesh.shape['data']

    def local_grads(x_rows, tgt_rows, w_lstm, b_lstm, w_vocab):
        rows, steps, hid = x_rows.shape
        tok = rows * steps
        x_tok = jnp.swapaxes(x_rows, 0, 1).reshape(tok, hid)
        tgt_rep = jnp.broadcast_to(jnp.swapaxes(tgt_rows, 0, 1).reshape(tok, 1), (tok, LANES))
        me = lax.axis_index('data')
        start = jnp.minimum(me * SHARD, VOCAB - SHARD)
        w_shard = lax.dynamic_slice(w_vocab, (0, start), (hid, SHARD))
        w_shard = jnp.where(me == ndev - 1, jnp.roll(w_shard, VOCAB - ndev * SHARD, axis=1), w_shard)
        u_all, coef, x_last = run_fwd(x_tok, w_lstm, b_lstm, steps, rows)
        x_all, stat_all, m_rep, r_rep = run_head(x_last, w_vocab, tgt_rep, ndev)
        dw, db, dx, dv = run_main(x_all, stat_all, w_vocab, w_shard, m_rep, r_rep, tgt_rep, x_last, u_all, coef, w_lstm, steps, rows, ndev)
        dx_rows = jnp.swapaxes(dx.reshape(steps, rows, hid), 0, 1)
        return dw, db, dv[:, :VOCAB], dx_rows

    return jax.shard_map(local_grads, mesh=mesh, in_specs=(P('data'), P('data'), P(), P(), P()), out_specs=(P(), P(), P(), P('data')), check_vma=False)
```

```python
import functools

import jax
import jax.numpy as jnp
from jax import lax
from jax.experimental import pallas as pl
from jax.experimental.pallas import tpu as pltpu
from jax.sharding import PartitionSpec as P

F32 = jnp.float32
BF16 = jnp.bfloat16
VMEM_CAP = 60 * 1024 * 1024
VOCAB_BLK = 1280
SHARD = 1024
VOCAB = 32000
LANES = 128
SUBL = 8
NSEM = 384
XPARTS = 2
XEARLY = 14


def mm(lhs, rhs, dims=((1,), (0,))):
    return lax.dot_general(lhs, rhs, (dims, ((), ())), preferred_element_type=F32)


def sig(val):
    return 0.5 * jnp.tanh(0.5 * val) + 0.5


MESH_ID = pl.DeviceIdType.MESH
SIDES = ((0, 1), (1, 0))
QUAD = ((0, 0), (0, 1), (1, 0), (1, 1))
FAR = (1, 2, 3)
HERE = (0, 0, 0, False)
LINE = (0, 1, 2, 3)


class Place:
    def __init__(self, me):
        self.me = me
        half, quarter = lax.div(me, 2), lax.div(me, 4)
        self.core, self.x, self.y, self.z = (
            lax.rem(me, 2), lax.rem(half, 2), lax.rem(quarter, 2), lax.div(me, 8))
        self.zs = [self.z, self.z + 1 - 2 * lax.rem(self.z, 2), lax.rem(self.z + 2, 4), 3 - self.z]
        self.at = {}
        for k in LINE:
            for fy, fx in QUAD:
                for other in (False, True):
                    y = 1 - self.y if fy else self.y
                    x = 1 - self.x if fx else self.x
                    c = 1 - self.core if other else self.core
                    self.at[k, fy, fx, other] = (self.zs[k], y, x, c)
        self.devs = {key: ((z * 2 + y) * 2 + x) * 2 + c for key, (z, y, x, c) in self.at.items()}
        self.partner = self.dev(0, 0, 0, True)

    def dev(self, k, fy, fx, other=False):
        return self.devs[k, fy, fx, other]

    def barrier(self):
        peers = [self.dev(k, 0, 0) for k in FAR] + [self.dev(0, *side) for side in SIDES] + [self.partner]
        sem = pltpu.get_barrier_semaphore()
        for peer in peers:
            pl.semaphore_signal(sem, device_id=(peer,), device_id_type=MESH_ID)
        pl.semaphore_wait(sem, len(peers))


class Link:
    def __init__(self, send, recv):
        self.send, self.recv, self.keys = send, recv, {}

    def copy(self, key, src, dst, peer):
        at = self.keys.setdefault(key, len(self.keys))
        return pltpu.make_async_remote_copy(
            src_ref=src, dst_ref=dst, send_sem=self.send.at[at], recv_sem=self.recv.at[at],
            device_id=(peer,), device_id_type=MESH_ID)


class Gather:
    def __init__(self, place, link, name, own, slot, half):
        self.p, self.link, self.name, self.own, self.slot, self.half = place, link, name, own, slot, half
        self.sent = []

    def _send(self, key, at, to, other=False, half=None):
        at = at + (False,)

        def make():
            if half is None:
                dst = self.slot(at)
                src = dst if any(at) else self.own
            else:
                src = dst = self.half(at, half)
            return self.link.copy((self.name,) + key, src, dst, self.p.dev(*to, other))

        self.sent.append(make)
        make().start()

    def _arrive(self, key, at, other=False, half=None):
        at = at + (other,)
        ref = self.slot(at) if half is None else self.half(at, half)
        self.link.copy((self.name,) + key, ref, ref, self.p.partner).wait_recv()

    def _pair(self, *at):
        self._send(('pair',) + at, at, LINE[:1] + QUAD[0], True)

    def _line(self, k):
        for side in SIDES:
            self._send(('line', k) + side, (k, 0, 0), (0,) + side)

    def _far(self):
        for k in FAR:
            self._send(('far', k), LINE[:1] + QUAD[0], (k,) + QUAD[0])

    def start(self):
        self._line(0)
        self._far()
        self._pair(0, 0, 0)

    def take_far(self, k):
        self._arrive(('far', k), (k,) + QUAD[0])
        self._line(k)
        self._pair(k, *QUAD[0])

    def take_line(self, k):
        for h, side in enumerate(SIDES):
            self._arrive(('line', k) + side, (k,) + side)
            self._send(('diag', k, h), (k,) + side, (0,) + SIDES[1 - h], half=h)
            self._pair(k, *side)

    def take_diag(self, k):
        for h in range(2):
            self._arrive(('diag', k, h), (k,) + QUAD[3], half=h)
        self._pair(k, *QUAD[3])

    def finish(self):
        for k in LINE:
            for side in QUAD:
                self._arrive(('pair', k) + side, (k,) + side, True)
        for make in self.sent:
            make().wait_send()

    def steps(self):
        far = [functools.partial(self.take_far, k) for k in LINE]
        line = [functools.partial(self.take_line, k) for k in LINE]
        diag = [functools.partial(self.take_diag, k) for k in LINE]
        return [far[1], line[0], far[2], line[1], far[3], diag[0], line[2], diag[1], line[3]] + diag[2:]


def fwd_kernel(steps, rows, hid, x_ref, w_ref, b_ref, u_ref, coef_ref, top_ref, xs, zin):
    layer = pl.program_id(0)

    @pl.when(layer == 0)
    def _():
        xs[...] = x_ref[...]

    x_val = xs[...]
    u_ref[0, :, :hid] = x_val
    zin[...] = mm(x_val, w_ref[0, :hid, :]) + b_ref[pl.ds(layer, 1), :]
    h_low = jnp.zeros((rows, hid), BF16)
    cell = jnp.zeros((rows, hid), F32)
    for step in range(steps):
        ts = pl.ds(step * rows, rows)
        u_ref[0, ts, hid:] = h_low
        z_all = zin[ts, :]
        if step:
            z_all = z_all + mm(h_low, w_ref[0, hid:, :])
        gi = sig(z_all[:, :hid])
        gf = sig(z_all[:, hid:2 * hid])
        gg = jnp.tanh(z_all[:, 2 * hid:3 * hid])
        go = sig(z_all[:, 3 * hid:])
        c_new = gf * cell + gi * gg
        tc = jnp.tanh(c_new)
        h_new = go * tc
        h_low = h_new.astype(BF16)
        coefs = (gg * gi * (1.0 - gi), cell * gf * (1.0 - gf), gi * (1.0 - gg * gg), tc * go * (1.0 - go),
                 go * (1.0 - tc * tc), gf)
        for at, val in enumerate(coefs):
            coef_ref[0, ts, at * hid:(at + 1) * hid] = val
        cell = c_new
        xs[ts, :] = (xs[ts, :].astype(F32) + h_new).astype(BF16)

    @pl.when(layer == pl.num_programs(0) - 1)
    def _():
        top_ref[...] = xs[...]


def run_fwd(x_tok, w_lstm, b_lstm, steps, rows):
    layers, _, wide = w_lstm.shape
    hid = wide // 4
    tok = steps * rows
    return pl.pallas_call(
        functools.partial(fwd_kernel, steps, rows, hid),
        grid=(layers,),
        in_specs=[
            pl.BlockSpec((tok, hid), lambda i: (0, 0)),
            pl.BlockSpec((1, 2 * hid, wide), lambda i: (i, 0, 0)),
            pl.BlockSpec((layers, wide), lambda i: (0, 0)),
        ],
        out_specs=[
            pl.BlockSpec((1, tok, 2 * hid), lambda i: (i, 0, 0)),
            pl.BlockSpec((1, tok, 6 * hid), lambda i: (i, 0, 0)),
            pl.BlockSpec((tok, hid), lambda i: (0, 0)),
        ],
        out_shape=[
            jax.ShapeDtypeStruct((layers, tok, 2 * hid), BF16),
            jax.ShapeDtypeStruct((layers, tok, 6 * hid), F32),
            jax.ShapeDtypeStruct((tok, hid), BF16),
        ],
        scratch_shapes=[pltpu.VMEM((tok, hid), BF16), pltpu.VMEM((tok, wide), F32)],
        compiler_params=pltpu.CompilerParams(vmem_limit_bytes=VMEM_CAP),
        name='lstm_fwd',
        cost_estimate=pl.CostEstimate(flops=70_000_000_000, bytes_accessed=40_000_000, transcendentals=0),
    )(x_tok, w_lstm, b_lstm)


def head_kernel(blk, x_ref, w_ref, tgt_ref, xall_ref, sall_ref, m_ref, r_ref, m_s, s_s, stat_s, ssem, rsem, lsem):
    blk_id = pl.program_id(0)
    last = pl.num_programs(0) - 1
    tok = x_ref.shape[0]
    place = Place(lax.axis_index('data'))
    link = Link(ssem, rsem)
    mid = tok // 2

    def chunk_at(part):
        num = tok // XPARTS
        row = lambda dev, h, n: pl.ds(pl.multiple_of(dev * tok + part * num + h * n, n), n)
        return Gather(place, link, ('x', part), x_ref.at[pl.ds(part * num, num), :],
                      lambda at: xall_ref.at[row(place.devs[at], 0, num), :],
                      lambda at, h: xall_ref.at[row(place.devs[at], h, num // 2), :])

    gats = [chunk_at(part) for part in range(XPARTS)]
    gat_s = Gather(place, link, 's', stat_s, lambda at: sall_ref.at[place.devs[at]],
                   lambda at, h: sall_ref.at[place.devs[at], :, pl.ds(h * mid, mid)])
    loc_x = [pltpu.make_async_copy(g.own, g.slot(HERE), lsem.at[1 + at]) for at, g in enumerate(gats)]
    loc_s = pltpu.make_async_copy(stat_s, gat_s.slot(HERE), lsem.at[0])
    sx, ss = [act for acts in zip(*[g.steps() for g in gats]) for act in acts], gat_s.steps()

    @pl.when(blk_id == 0)
    def _():
        place.barrier()
        for gat, loc in zip(gats, loc_x):
            gat.start()
            loc.start()
        m_s[...] = jnp.full(m_s.shape, -jnp.inf, F32)
        s_s[...] = jnp.zeros(s_s.shape, F32)

    for at, act in zip(range(6, VOCAB // blk - 1), sx[:XEARLY]):
        pl.when(blk_id == at)(act)

    logits = mm(x_ref[...], w_ref[...])
    cols = [logits[:, k:k + LANES] for k in range(0, blk, LANES)]
    m_old = m_s[...]
    m_new = functools.reduce(jnp.maximum, cols, m_old)
    tot = s_s[...] * jnp.exp(m_old - m_new)
    for col in cols:
        tot = tot + jnp.exp(col - m_new)
    m_s[...] = m_new
    s_s[...] = tot

    @pl.when(blk_id == last)
    def _():
        m_lane = m_s[...]
        m_row = jnp.max(m_lane, axis=1, keepdims=True)
        s_row = jnp.sum(s_s[...] * jnp.exp(m_lane - m_row), axis=1, keepdims=True)
        m_rep = jnp.broadcast_to(m_row, m_lane.shape)
        r_rep = jnp.broadcast_to(1.0 / s_row, m_lane.shape)
        m_ref[...] = m_rep
        r_ref[...] = r_rep
        stat_s[...] = jnp.zeros(stat_s.shape, F32)
        for at, val in enumerate((m_rep, r_rep, tgt_ref[...].astype(F32))):
            stat_s[at:at + 1, :] = val.T[:1, :]
        gat_s.start()
        loc_s.start()
        for at in range(len(ss)):
            for act in sx[XEARLY + at:XEARLY + at + 1] + ss[at:at + 1]:
                act()
        for act in sx[XEARLY + len(ss):]:
            act()
        for gat in gats + [gat_s]:
            gat.finish()
        for loc in loc_x + [loc_s]:
            loc.wait()


def run_head(x_top, w_vocab, tgt_rep, ndev):
    tok, hid = x_top.shape
    full = pl.BlockSpec(memory_space=pltpu.VMEM)
    anyw = pl.BlockSpec(memory_space=pl.ANY)
    stat = jax.ShapeDtypeStruct((tok, LANES), F32)
    same = pl.BlockSpec((tok, LANES), lambda j: (0, 0))
    return pl.pallas_call(
        functools.partial(head_kernel, VOCAB_BLK),
        grid=(VOCAB // VOCAB_BLK,),
        in_specs=[full, pl.BlockSpec((hid, VOCAB_BLK), lambda j: (0, j)), full],
        out_specs=[anyw, anyw, same, same],
        out_shape=[
            jax.ShapeDtypeStruct((ndev * tok, hid), BF16),
            jax.ShapeDtypeStruct((ndev, SUBL, tok), F32), stat, stat,
        ],
        scratch_shapes=[
            pltpu.VMEM((tok, LANES), F32), pltpu.VMEM((tok, LANES), F32), pltpu.VMEM((SUBL, tok), F32),
            pltpu.SemaphoreType.DMA((LANES,)), pltpu.SemaphoreType.DMA((LANES,)), pltpu.SemaphoreType.DMA((1 + XPARTS,)),
        ],
        compiler_params=pltpu.CompilerParams(vmem_limit_bytes=VMEM_CAP, collective_id=1, has_side_effects=True),
        name='head',
        cost_estimate=pl.CostEstimate(flops=10**10, bytes_accessed=10**7, transcendentals=0),
    )(x_top, w_vocab, tgt_rep)


GROUP = 2
SPLIT = 4
WID = SHARD // SPLIT
TOK_BLK = 2048
PACE = (6, 8)
TAKES = ((0, 2, 4, 6), (3, 5, 7, 9), (6, 8, 10, 12), (9, 11, 13, 15))


class Reduce:
    def __init__(self, place, link, grp, buf, boxes):
        self.p, self.link, self.grp, self.buf, self.boxes = place, link, grp, buf, boxes
        self.first = grp * GROUP
        self.lay = pl.ds(self.first, GROUP)
        p = place
        xdev, ydev = p.dev(0, *SIDES[0]), p.dev(0, *SIDES[1])
        pick = lambda one, two: (1 - p.core) * one + p.core * two
        self.peers = [p.partner, pick(xdev, ydev), pick(ydev, xdev)]
        self.give, self.keep, self.size, base = [], [], [], 0
        for at, bit in enumerate((p.core, pick(p.x, p.y), pick(p.y, p.x))):
            size = buf.shape[1] >> (at + 1)
            self.size.append(size)
            self.give.append(base + (1 - bit) * size)
            base = base + bit * size
            self.keep.append(base)
        self.unit = size // len(LINE)
        self.base = base
        self.sent = []

    def _rows(self, start, num):
        return pl.ds(pl.multiple_of(start, num), num)

    def _copies(self, at):
        if at < len(self.size):
            src = self.buf.at[self.lay, self._rows(self.give[at], self.size[at]), :]
            return [self.link.copy(('sum', self.grp, at), src, self.boxes[at].at[self.lay], self.peers[at])]
        out = []
        for k in FAR:
            src = self.buf.at[self.lay, self._rows(self.base + self.p.zs[k] * self.unit, self.unit), :]
            dst = self.boxes[at].at[k - 1, self.lay]
            out.append(self.link.copy(('sum', self.grp, at, k), src, dst, self.p.dev(k, 0, 0)))
        return out

    def start(self, at=0):
        for copy in self._copies(at):
            copy.start()

    def take(self, at):
        for copy in self._copies(at):
            copy.wait_recv()
        far = at == len(self.size)
        num = self.unit if far else self.size[at]
        rows = self._rows(self.base + self.p.z * num if far else self.keep[at], num)
        for i in range(GROUP):
            lay = self.first + i
            val = self.buf[lay, rows, :]
            for k in FAR if far else FAR[:1]:
                val = val + (self.boxes[at][k - 1, lay] if far else self.boxes[at][lay])
            self.buf[lay, rows, :] = val
        if not far:
            self.start(at + 1)

    def finish(self):
        for at in LINE:
            for copy in self._copies(at):
                copy.wait_send()


def main_kernel(phases, steps, rows, hid, x_ref, stat_ref, wv_ref, wsh_ref, m_ref, r_ref, tgt_ref, xl_ref,
                u_ref, coef_ref, w_ref, dw_ref, db_ref, dx_ref, dv_ref,
                wt, acc, shv, dx, dz_s, wrt, dbp, buf, r0, r1, r2, r3, dbb, dball, gs, gr, ls):
    step_id = pl.program_id(0)
    n_vocab, n_top, n_layers = phases
    t_top = n_vocab
    t_bwd = n_vocab + n_top
    t_last = t_bwd + n_layers - 1
    place = Place(lax.axis_index('data'))
    link = Link(gs, gr)
    ndev = stat_ref.shape[0] * n_vocab // SPLIT
    tail = dball.shape[0] - 1

    def chunk_at(q):
        cols = lambda at: pl.ds(pl.multiple_of(place.devs[at] * SHARD + q * WID, WID), WID)
        return Gather(
            place, link, ('v', q), shv.at[q], lambda at: dv_ref.at[:, cols(at)],
            lambda at, h: dv_ref.at[pl.ds(h * (hid // 2), hid // 2), cols(at)])

    def piece(at):
        z, y, x, c = place.at[at]
        far, near = hid // 2, hid // 4
        return c * hid + ((1 - c) * x + c * y) * far + ((1 - c) * y + c * x) * near + z * (near // 4)

    pieces = {at: piece(at) for at in place.at}

    def group_at(grp):
        lay = pl.ds(grp * GROUP, GROUP)
        unit = hid // 16
        part = lambda at, h, n: pl.ds(pl.multiple_of(pieces[at] + h * n, n), n)
        return Gather(
            place, link, ('w', grp), buf.at[lay, part(HERE, 0, unit), :],
            lambda at: dw_ref.at[lay, part(at, 0, unit), :],
            lambda at, h: dw_ref.at[lay, part(at, h, unit // 2), :])

    gats = [chunk_at(q) for q in range(SPLIT)]
    n_grp = n_layers // GROUP
    reds = [Reduce(place, link, n_grp - 1 - j, buf, (r0, r1, r2, r3)) for j in range(n_grp)]
    outs = [group_at(n_grp - 1 - j) for j in range(n_grp)]
    wide2 = dbb.shape[1] // 2
    gdb = Gather(place, link, 'b', dbb, lambda at: dball.at[place.devs[at]],
                 lambda at, h: dball.at[place.devs[at], :, pl.ds(h * wide2, wide2)])
    own_v = [pltpu.make_async_copy(shv.at[q], gats[q].slot(HERE), ls.at[q]) for q in range(SPLIT)]
    own_w = [pltpu.make_async_copy(outs[g].own, outs[g].slot(HERE), ls.at[SPLIT + g]) for g in range(n_grp)]
    def slot_of(when):
        return when if when < t_bwd else t_bwd + (when - t_bwd) // 6

    per_chunk = n_vocab // SPLIT
    todo = sorted(
        (per_chunk * (q + 1) + PACE[0] + PACE[1] * n, q, n) for q in range(SPLIT) for n in range(len(gats[q].steps())))
    acts = [(slot_of(when), gats[q].steps()[n]) for when, q, n in todo]

    def emit(j):
        reds[j].take(3)
        outs[j].start()
        own_w[j].start()

    late = []
    for j, when in enumerate(TAKES):
        ops = [functools.partial(reds[j].take, n) for n in range(3)] + [functools.partial(emit, j)]
        late += [(when[n], j, op) for n, op in enumerate(ops)]
        late += [(when[-1] + 4 * n + 1, j, op) for n, op in enumerate(outs[j].steps())]
    late += [(TAKES[1][-1] + 4 * n + 3, n_grp, op) for n, op in enumerate(gdb.steps())]
    late = [op for _, _, op in sorted(late, key=lambda item: item[:2])]

    @pl.when(step_id == 0)
    def _():
        place.barrier()
        wt[...] = wsh_ref[...].T
        dx[...] = jnp.zeros(dx.shape, F32)

    per = n_vocab // SPLIT
    q_now, blk_now = lax.div(step_id, per), lax.rem(step_id, per)

    @pl.when((step_id < t_top) & (blk_now == 0))
    def _():
        acc[...] = jnp.zeros(acc.shape, F32)

    @pl.when(step_id < t_top)
    def _():
        m_row, r_row, tgt = [
            jnp.concatenate([stat_ref[p, r:r + 1, :] for p in range(stat_ref.shape[0])], axis=1) for r in range(3)]
        x_val = x_ref[...]
        logits = mm(wt[pl.ds(pl.multiple_of(q_now * WID, WID), WID), :], x_val, ((1,), (1,)))
        prob = jnp.exp(logits - m_row) * r_row
        ids = lax.broadcasted_iota(jnp.int32, prob.shape, 0) + (place.me * SHARD + q_now * WID)
        dist = ids.astype(F32) - tgt
        hot = jnp.maximum(1.0 - dist * dist, 0.0)
        acc[...] += mm((prob - hot).astype(BF16), x_val)

    for k in range(SPLIT):
        @pl.when(step_id == k * per + per - 1)
        def _(k=k):
            shv[k] = acc[...].T
            gats[k].start()
            own_v[k].start()

    for at, act in acts:
        if at < t_last:
            pl.when(step_id == at)(act)

    @pl.when((step_id >= t_top) & (step_id < t_bwd))
    def _():
        blk = wv_ref.shape[1]
        logits = mm(xl_ref[...], wv_ref[...])
        m_row, r_row = m_ref[...], r_ref[...]
        off = tgt_ref[...] - (lax.broadcasted_iota(jnp.int32, m_row.shape, 1) + (step_id - t_top) * blk)
        pieces = []
        for k in range(0, blk, LANES):
            prob = jnp.exp(logits[:, k:k + LANES] - m_row) * r_row
            pieces.append(jnp.where(off == k, prob - 1.0, prob).astype(BF16))
        dx[...] += mm(jnp.concatenate(pieces, axis=1), wv_ref[...], ((1,), (1,)))

    @pl.when(step_id >= t_bwd)
    def _():
        lay = t_last - step_id
        wrt[...] = w_ref[0, hid:, :].T
        dbp[...] = jnp.zeros(dbp.shape, F32)
        e_rec = jnp.zeros((rows, hid), F32)
        dc_rec = jnp.zeros((rows, hid), F32)
        for step in reversed(range(steps)):
            ts = pl.ds(step * rows, rows)
            coef = [coef_ref[0, ts, at * hid:(at + 1) * hid] for at in range(6)]
            err = dx[ts, :] + e_rec
            dct = dc_rec + err * coef[4]
            e_rec = jnp.zeros((rows, hid), F32)
            for gate in LINE:
                cols = pl.ds(gate * hid, hid)
                dz = (err if gate == LINE[-1] else dct) * coef[gate]
                low = dz.astype(BF16)
                dz_s[ts, cols] = low
                if step:
                    e_rec = e_rec + mm(low, wrt[cols, :])
                dbp[:, cols] += functools.reduce(jnp.add, [dz[k:k + SUBL] for k in range(0, rows, SUBL)])
            dc_rec = dct * coef[5]
        dbb[pl.ds(lay, 1), :] = jnp.sum(dbp[...], axis=0, keepdims=True)
        dz_all = dz_s[...]
        buf[lay] = mm(u_ref[0], dz_all, ((0,), (0,)))
        dx[...] += mm(dz_all, w_ref[0, :hid, :], ((1,), (1,)))

    for j in range(n_grp):
        pl.when(step_id == t_bwd + GROUP * (j + 1) - 1)(reds[j].start)

    done = 0
    for at, upto in ((2, 1), (4, 3), (6, 4)):
        for act in late[done:upto]:
            pl.when(step_id == t_bwd + at)(act)
        done = upto

    @pl.when(step_id == t_last)
    def _():
        dx_ref[...] = dx[...]
        gdb.start()
        rest = [act for at, act in acts if at >= t_last]
        for at in range(len(late) - done):
            for act in rest[at:at + 1] + late[done + at:done + at + 1]:
                act()
        for act in rest[len(late) - done:]:
            act()
        dball[place.me] = dbb[...]
        gdb.finish()
        total = dball[0]
        for dev in range(1, tail + 1):
            total = total + dball[dev]
        db_ref[...] = total
        for gat in gats + outs:
            gat.finish()
        for q in range(SPLIT):
            own_v[q].wait()
        for copy in own_w:
            copy.wait()
        for red in reds:
            red.finish()


def run_main(x_all, stat_all, w_vocab, w_shard, m_rep, r_rep, tgt_rep, x_last, u_all, coef, w_lstm, steps, rows, ndev):
    layers, _, wide = w_lstm.shape
    hid = wide // 4
    tok = steps * rows
    blocks = ndev * tok // TOK_BLK
    phases = (SPLIT * blocks, VOCAB // VOCAB_BLK, layers)
    t_top = phases[0]
    t_bwd = t_top + phases[1]
    full = pl.BlockSpec(memory_space=pltpu.VMEM)
    anyw = pl.BlockSpec(memory_space=pl.ANY)
    total = sum(phases)
    past = lambda i, at: (i + total - at) // total
    at_tok = lambda i: (1 - past(i, t_top)) * (i % blocks) + past(i, t_top) * (blocks - 1)
    at_voc = lambda i: past(i, t_top) * (1 - past(i, t_bwd)) * (i - t_top) + past(i, t_bwd) * (phases[1] - 1)
    at_lay = lambda i: layers - 1 - past(i, t_bwd) * (i - t_bwd)
    same = lambda shape: pl.BlockSpec(shape, lambda i: (0, 0))
    sem = pltpu.SemaphoreType.DMA
    return pl.pallas_call(
        functools.partial(main_kernel, phases, steps, rows, hid),
        grid=(total,),
        in_specs=[
            pl.BlockSpec((TOK_BLK, hid), lambda i: (at_tok(i), 0)),
            pl.BlockSpec((TOK_BLK // tok, SUBL, tok), lambda i: (at_tok(i), 0, 0)),
            pl.BlockSpec((hid, VOCAB_BLK), lambda i: (0, at_voc(i))),
            full, full, full, full, full,
            pl.BlockSpec((1, tok, 2 * hid), lambda i: (at_lay(i), 0, 0)),
            pl.BlockSpec((1, tok, 6 * hid), lambda i: (at_lay(i), 0, 0)),
            pl.BlockSpec((1, 2 * hid, wide), lambda i: (at_lay(i), 0, 0)),
        ],
        out_specs=[anyw, same((layers, wide)), same((tok, hid)), anyw],
        out_shape=[
            jax.ShapeDtypeStruct((layers, 2 * hid, wide), F32),
            jax.ShapeDtypeStruct((layers, wide), F32),
            jax.ShapeDtypeStruct((tok, hid), F32),
            jax.ShapeDtypeStruct((hid, ndev * SHARD), F32),
        ],
        scratch_shapes=[
            pltpu.VMEM((SHARD, hid), BF16),
            pltpu.VMEM((WID, hid), F32),
            pltpu.VMEM((SPLIT, hid, WID), F32),
            pltpu.VMEM((tok, hid), F32),
            pltpu.VMEM((tok, wide), BF16),
            pltpu.VMEM((wide, hid), BF16),
            pltpu.VMEM((SUBL, wide), F32),
            pltpu.VMEM((layers, 2 * hid, wide), F32),
            pltpu.VMEM((layers, hid, wide), F32),
            pltpu.VMEM((layers, hid // 2, wide), F32),
            pltpu.VMEM((layers, hid // 4, wide), F32),
            pltpu.VMEM((3, layers, hid // 16, wide), F32),
            pltpu.VMEM((layers, wide), F32),
            pltpu.VMEM((ndev, layers, wide), F32),
            sem((NSEM,)), sem((NSEM,)), sem((SPLIT + layers // GROUP,)),
        ],
        compiler_params=pltpu.CompilerParams(vmem_limit_bytes=VMEM_CAP, collective_id=2, has_side_effects=True),
        name='main',
        cost_estimate=pl.CostEstimate(flops=10**10, bytes_accessed=10**7, transcendentals=0),
    )(x_all, stat_all, w_vocab, w_shard, m_rep, r_rep, tgt_rep, x_last, u_all, coef, w_lstm)


def solution(mesh):
    ndev = mesh.shape['data']

    def local_grads(x_rows, tgt_rows, w_lstm, b_lstm, w_vocab):
        rows, steps, hid = x_rows.shape
        tok = rows * steps
        x_tok = jnp.swapaxes(x_rows, 0, 1).reshape(tok, hid)
        tgt_rep = jnp.broadcast_to(jnp.swapaxes(tgt_rows, 0, 1).reshape(tok, 1), (tok, LANES))
        me = lax.axis_index('data')
        start = jnp.minimum(me * SHARD, VOCAB - SHARD)
        w_shard = lax.dynamic_slice(w_vocab, (0, start), (hid, SHARD))
        w_shard = jnp.where(me == ndev - 1, jnp.roll(w_shard, VOCAB - ndev * SHARD, axis=1), w_shard)
        u_all, coef, x_last = run_fwd(x_tok, w_lstm, b_lstm, steps, rows)
        x_all, stat_all, m_rep, r_rep = run_head(x_last, w_vocab, tgt_rep, ndev)
        dw, db, dx, dv = run_main(x_all, stat_all, w_vocab, w_shard, m_rep, r_rep, tgt_rep, x_last, u_all, coef, w_lstm, steps, rows, ndev)
        dx_rows = jnp.swapaxes(dx.reshape(steps, rows, hid), 0, 1)
        return dw, db, dv[:, :VOCAB], dx_rows

    return jax.shard_map(local_grads, mesh=mesh, in_specs=(P('data'), P('data'), P(), P(), P()), out_specs=(P(), P(), P(), P('data')), check_vma=False)
```
